32 devices in a mesh: dp: 4 (over x, core), tensor: 8 (over z, y).
Axes of the slice: x: 2, y: 2, z: 4, core: 2. Of those that a mesh axis runs over, the one named last changes fastest.
Arguments:
- tokens: bfloat16 [96, 8, 4096], P('dp'), may hold values from -6 to 6
- norm_gain: float32 [4096], replicated, may hold values from 0.1 to 1.9
- in_weight: bfloat16 [4096, 2, 4096], P(None, None, 'tensor'), may hold values from -0.09375 to 0.09375
- group_weight: bfloat16 [4096, 1024], P(None, 'tensor'), may hold values from -0.09375 to 0.09375
- step_weight: bfloat16 [4096, 64], P(None, 'tensor'), may hold values from -0.09375 to 0.09375
- value_kernel: bfloat16 [4, 4096], P(None, 'tensor'), may hold values from -3 to 3
- value_offset: bfloat16 [4096], P('tensor'), may hold values from -3 to 3
- group_kernel: bfloat16 [4, 1024], P(None, 'tensor'), may hold values from -3 to 3
- group_offset: bfloat16 [1024], P('tensor'), may hold values from -3 to 3
- step_bias: float32 [64], P('tensor'), may hold values from -4 to 1
- decay_rate: float32 [64], P('tensor'), may hold values from 0.05 to 2
- skip_gain: float32 [64], P('tensor'), may hold values from 0.5 to 2
- out_gain: float32 [4096], P('tensor'), may hold values from 0.1 to 1.9
- out_weight: bfloat16 [4096, 4096], P('tensor'), may hold values from -0.09375 to 0.09375
- scan_state: bfloat16 [96, 64, 64, 128], P('dp', 'tensor'), may hold values from -6 to 6
- value_cache: bfloat16 [96, 3, 4096], P('dp', None, 'tensor'), may hold values from -6 to 6
- group_cache: bfloat16 [96, 3, 1024], P('dp', None, 'tensor'), may hold values from -6 to 6
- accepted: int32 [96], P('dp'), may hold values from 0 to 8, as said below
- draft_lengths: int32 [96], P('dp'), may hold values from 1 to 8, as said below
- live_flags: int32 [96], P('dp'), may hold values 0 or 1
Outputs:
- layer_out: bfloat16 [96, 8, 4096], P('dp')
- kept_state: bfloat16 [96, 64, 64, 128], P('dp', 'tensor')
- value_kept: bfloat16 [96, 3, 4096], P('dp', None, 'tensor')
- group_kept: bfloat16 [96, 3, 1024], P('dp', None, 'tensor')
- accepted_total: int32 [1], replicated
The draws below stay inside these ranges and needn't reach their ends.
Inputs may be any that keep to these rules, and one draw needn't show every extreme that they name: `draft_lengths`: positions at or after a request's draft length are padding. `accepted`: never more than the same request's draft length.
All inputs are finite; a program needn't handle non-finite values.
Results may differ from the reference program's by a relative error of at most 0.012.
Values may be sent and summed in bfloat16 or wider, within the bound.
A program may use at most 128 MiB of HBM per device.

```python
import math
import jax
import jax.numpy as jnp
from jax import lax

D = 4096
STATE = 128
HEADDIM = 64
CONV = 4
DRAFT = 8
REQ_DEV = 24
HEADS = 64
NGROUPS = 4
INNER = 4096
GCOLS = 1024
REQUESTS = 96


def draft_pair(key):
    block_count = REQUESTS // REQ_DEV
    full_row = jax.random.randint(jax.random.fold_in(key, 10), (), 0, REQUESTS)
    short_row = (full_row + 1) % REQUESTS
    block_caps = jax.random.randint(jax.random.fold_in(key, 11), (block_count,), 1, DRAFT + 1)
    block_caps = jnp.where(jnp.arange(block_count) == full_row // REQ_DEV, DRAFT, block_caps)
    per_request = jnp.repeat(block_caps, REQ_DEV, total_repeat_length=REQUESTS)
    lengths = jax.random.randint(jax.random.fold_in(key, 12), (REQUESTS,), 1, per_request + 1)
    row_ids = jnp.arange(REQUESTS)
    lengths = jnp.where(row_ids == full_row, DRAFT, lengths)
    lengths = jnp.where(row_ids == short_row, 1, lengths)
    accepted_counts = jax.random.randint(jax.random.fold_in(key, 13), (REQUESTS,), 0, lengths + 1)
    accepted_counts = jnp.where(row_ids == full_row, DRAFT, accepted_counts)
    accepted_counts = jnp.where(row_ids == short_row, 0, accepted_counts)
    return (lengths.astype(jnp.int32), accepted_counts.astype(jnp.int32))


def draw_draft_lengths(key, part):
    return draft_pair(key)[0]


def draw_accepted(key, part):
    return draft_pair(key)[1]


def plant(array, own_key, smallest, largest):
    extent = array.shape
    index_at = [jax.random.randint(jax.random.fold_in(own_key, axis), (), 0, extent[axis]) for axis in range(len(extent))]
    array = array.at[tuple(index_at)].set(smallest)
    longest = extent.index(max(extent))
    index_at[longest] = (index_at[longest] + 1) % extent[longest]
    return array.at[tuple(index_at)].set(largest)


def block_levels(own_key, dims, cuts, smallest, top_value):
    factor_of, own = 1.0, jax.random.fold_in(own_key, 6)
    for dim, blocks in cuts:
        draws = jnp.exp(jax.random.uniform(jax.random.fold_in(own, dim), (blocks,), jnp.float32, smallest / len(cuts), top_value / len(cuts)))
        factor_of = factor_of * jnp.repeat(draws, dims[dim] // blocks).reshape([-1 if axis == dim else 1 for axis in range(len(dims))])
    return factor_of


def noise(own_key, dims, deviation, most, cuts=(), kind=jnp.bfloat16):
    factor_of = block_levels(own_key, dims, cuts, -0.22, 0.18) if cuts else 1.0
    result = jax.random.normal(own_key, dims, jnp.float32) * deviation * factor_of
    return jnp.minimum(jnp.maximum(result, -most), most).astype(kind)


def setup_inputs(seed: int = 0) -> dict:
    arg_keys = jax.random.split(jax.random.key(seed), 21)
    tokens = noise(arg_keys[0], (REQUESTS, DRAFT, D), 1.0, 6.0, ((0, 4),))
    norm_gain = jnp.clip(1.0 + 0.18 * jax.random.normal(arg_keys[1], (D,), jnp.float32), 0.1, 1.9)
    in_weight = noise(arg_keys[2], (D, 2, INNER), D ** -0.5, 0.09375, ((2, 8),))
    group_weight = noise(arg_keys[3], (D, GCOLS), D ** -0.5, 0.09375, ((1, 8),))
    step_weight = noise(arg_keys[4], (D, HEADS), D ** -0.5, 0.09375, ((1, 8),))
    value_kernel = noise(arg_keys[5], (CONV, INNER), CONV ** -0.5, 3.0, ((1, 8),))
    value_offset = noise(arg_keys[6], (INNER,), 0.5, 3.0, ((0, 8),))
    group_kernel = noise(arg_keys[7], (CONV, GCOLS), CONV ** -0.5, 3.0, ((1, 8),))
    group_offset = noise(arg_keys[8], (GCOLS,), 0.5, 3.0, ((0, 8),))
    step_bias = jnp.clip(-4.0 + 5.0 * jax.random.uniform(arg_keys[9], (HEADS,), jnp.float32) ** block_levels(arg_keys[9], (HEADS,), ((0, 8),), -0.2, 0.2), -4.0, 1.0)
    decay_rate = jnp.clip(jnp.exp(math.log(2.0) - 3.6888794 * jax.random.uniform(arg_keys[10], (HEADS,), jnp.float32) ** block_levels(arg_keys[10], (HEADS,), ((0, 8),), -0.2, 0.2)), 0.05, 2.0)
    skip_gain = jnp.clip(0.5 + 1.5 * jax.random.uniform(arg_keys[11], (HEADS,), jnp.float32) ** block_levels(arg_keys[11], (HEADS,), ((0, 8),), -0.2, 0.2), 0.5, 2.0)
    out_gain = jnp.clip(1.0 + 0.18 * jax.random.normal(arg_keys[12], (INNER,), jnp.float32), 0.1, 1.9)
    out_weight = noise(arg_keys[13], (INNER, D), INNER ** -0.5, 0.09375, ((0, 8),))
    scan_state = noise(arg_keys[14], (REQUESTS, HEADS, HEADDIM, STATE), 1.0, 6.0, ((0, 4), (1, 8)))
    value_cache = noise(arg_keys[15], (REQUESTS, CONV - 1, INNER), 1.0, 6.0, ((0, 4), (2, 8)))
    group_cache = noise(arg_keys[16], (REQUESTS, CONV - 1, GCOLS), 1.0, 6.0, ((0, 4), (2, 8)))
    accepted = draw_accepted(jax.random.fold_in(arg_keys[20], 71), 0)
    draft_lengths = draw_draft_lengths(jax.random.fold_in(arg_keys[20], 71), 0)
    live_flags = plant((jax.random.randint(arg_keys[19], (REQUESTS,), 0, 8) < 7).astype(jnp.int32), jax.random.fold_in(arg_keys[19], 1), 0, 1)
    return {"tokens": tokens, "norm_gain": norm_gain, "in_weight": in_weight, "group_weight": group_weight, "step_weight": step_weight, "value_kernel": value_kernel, "value_offset": value_offset, "group_kernel": group_kernel, "group_offset": group_offset, "step_bias": step_bias, "decay_rate": decay_rate, "skip_gain": skip_gain, "out_gain": out_gain, "out_weight": out_weight, "scan_state": scan_state, "value_cache": value_cache, "group_cache": group_cache, "accepted": accepted, "draft_lengths": draft_lengths, "live_flags": live_flags}


EPSILON = 1e-05

def convolve(window, fresh_rows, kernel, offset):
    sequence = jnp.concatenate([window, fresh_rows], axis=1)
    length = fresh_rows.shape[1]
    summed = jnp.zeros(fresh_rows.shape, jnp.float32) + offset.astype(jnp.float32)
    for tap_index in range(kernel.shape[0]):
        summed = summed + kernel[tap_index].astype(jnp.float32) * sequence[:, tap_index:tap_index + length].astype(jnp.float32)
    return (jax.nn.silu(summed), sequence)

def keep_window(sequence, kept_count, width_rows):
    return jax.vmap(lambda single, start_row: lax.dynamic_slice_in_dim(single, start_row, width_rows, 0))(sequence, kept_count)

def reference(tokens, norm_gain, in_weight, group_weight, step_weight, value_kernel, value_offset, group_kernel, group_offset, step_bias, decay_rate, skip_gain, out_gain, out_weight, scan_state, value_cache, group_cache, accepted, draft_lengths, live_flags):
    flat_rows = tokens.reshape(REQUESTS * DRAFT, D).astype(jnp.float32)
    normed = (flat_rows * lax.rsqrt(lax.optimization_barrier(jnp.mean(flat_rows * flat_rows, axis=1, keepdims=True)) + EPSILON) * norm_gain).astype(jnp.bfloat16)
    inner_proj = jnp.dot(normed, in_weight.reshape(D, 2 * INNER), preferred_element_type=jnp.float32).astype(jnp.bfloat16).reshape(REQUESTS, DRAFT, 2, INNER)
    gate_part = inner_proj[:, :, 0]
    value_part = inner_proj[:, :, 1]
    group_proj = jnp.dot(normed, group_weight, preferred_element_type=jnp.float32).astype(jnp.bfloat16).reshape(REQUESTS, DRAFT, GCOLS)
    step_raw = jnp.dot(normed, step_weight, preferred_element_type=jnp.float32).reshape(REQUESTS, DRAFT, HEADS)
    value_conv, value_seq = convolve(value_cache, value_part, value_kernel, value_offset)
    group_conv, group_seq = convolve(group_cache, group_proj, group_kernel, group_offset)
    group_maps = group_conv.reshape(REQUESTS, DRAFT, NGROUPS, 2, STATE)
    input_maps = group_maps[:, :, :, 0]
    output_maps = group_maps[:, :, :, 1]
    step_size = jax.nn.softplus(step_raw + step_bias)
    decay_step = jnp.exp(-step_size * decay_rate)
    kept_count = accepted * live_flags
    per_group = HEADS // NGROUPS

    def head_scan(head_index):
        values = lax.dynamic_slice_in_dim(value_conv, head_index * HEADDIM, HEADDIM, 2)
        group_index = head_index // per_group
        input_map = lax.dynamic_index_in_dim(input_maps, group_index, 2, keepdims=False)
        output_map = lax.dynamic_index_in_dim(output_maps, group_index, 2, keepdims=False)
        head_decay = lax.dynamic_index_in_dim(decay_step, head_index, 2, keepdims=False)
        head_step = lax.dynamic_index_in_dim(step_size, head_index, 2, keepdims=False)
        initial = lax.dynamic_index_in_dim(scan_state, head_index, 1, keepdims=False).astype(jnp.float32)
        head_skip = lax.dynamic_index_in_dim(skip_gain, head_index, 0, keepdims=False)

        def advance(carry_pair, position):
            current, kept_now = carry_pair
            scaled = (head_step[:, position][:, None] * values[:, position])[:, :, None]
            current = head_decay[:, position][:, None, None] * current + scaled * input_map[:, position][:, None, :]
            produced = lax.optimization_barrier(jnp.sum(current * output_map[:, position][:, None, :], axis=2)) + head_skip * values[:, position]
            kept_now = jnp.where((position < kept_count)[:, None, None], current, kept_now)
            return ((current, kept_now), produced)
        (final_state, kept_now), produced = lax.scan(advance, (initial, initial), jnp.arange(DRAFT, dtype=jnp.int32))
        return (produced, kept_now.astype(jnp.bfloat16))
    produced, kept_heads = lax.map(head_scan, jnp.arange(HEADS, dtype=jnp.int32))
    head_out = jnp.transpose(produced, (2, 1, 0, 3)).reshape(REQUESTS, DRAFT, INNER)
    kept_state = jnp.transpose(kept_heads, (1, 0, 2, 3))
    gated = head_out * jax.nn.silu(gate_part.astype(jnp.float32))
    grouped = gated.reshape(REQUESTS, DRAFT, NGROUPS, INNER // NGROUPS)
    scale_rows = lax.rsqrt(lax.optimization_barrier(jnp.mean(grouped * grouped, axis=3, keepdims=True)) + EPSILON)
    valid_rows = (jnp.arange(DRAFT)[None, :] < draft_lengths[:, None]) & (live_flags[:, None] == 1)
    normalized = jnp.where(valid_rows[:, :, None], (grouped * scale_rows).reshape(REQUESTS, DRAFT, INNER) * out_gain, 0.0).astype(jnp.bfloat16)
    layer_out = jnp.dot(normalized.reshape(REQUESTS * DRAFT, INNER), out_weight, preferred_element_type=jnp.float32).astype(jnp.bfloat16).reshape(REQUESTS, DRAFT, D)
    value_kept = keep_window(value_seq, kept_count, CONV - 1)
    group_kept = keep_window(group_seq, kept_count, CONV - 1)
    accepted_total = jnp.sum(kept_count).astype(jnp.int32).reshape(1)
    return (layer_out, kept_state, value_kept, group_kept, accepted_total)
```

```python
import jax
import jax.numpy as jnp
from jax import lax
from jax.experimental import pallas as pl
from jax.experimental.pallas import tpu as pltpu
from jax.sharding import PartitionSpec as P

EPSILON = 1e-05


def narrow(value):
    return value.astype(jnp.bfloat16)


def swapped(value, axis, distance):
    mask = 2**distance
    pairs = [(source, source ^ mask) for source in range(lax.axis_size(axis))]
    return lax.ppermute(value, axis, pairs)


def total_over_dp(own):
    members = lax.axis_size("dp")
    total = own
    for hop in range(1, members):
        pairs = [(source, (source + hop) % members) for source in range(members)]
        total = total + lax.ppermute(own, "dp", pairs)
    return total


def convolve(window, fresh_rows, kernel, offset):
    sequence = jnp.concatenate([window, fresh_rows], axis=1)
    length = fresh_rows.shape[1]
    summed = jnp.zeros(fresh_rows.shape, jnp.float32) + offset.astype(jnp.float32)
    for tap_index in range(kernel.shape[0]):
        summed = summed + kernel[tap_index].astype(jnp.float32) * sequence[
            :, tap_index : tap_index + length
        ].astype(jnp.float32)
    return (jax.nn.silu(summed), sequence)


def keep_window(sequence, kept_count, width_rows):
    return jax.vmap(
        lambda single, start_row: lax.dynamic_slice_in_dim(single, start_row, width_rows, 0)
    )(sequence, kept_count)


MESH = pl.DeviceIdType.MESH


def project_kernel(
    normalized_ref,
    weight_ref,
    out_ref,
    weight_buf,
    pair_send,
    pair_recv,
    far_send,
    far_recv,
    kept_acc,
    weight_sem,
    pair_sems,
    far_sems,
    pair_out_sems,
    far_out_sems,
):
    members = lax.axis_size("tensor")
    fars = members // 2
    me = lax.axis_index("tensor")
    far, near = me // 2, me % 2
    partner = far * 2 + (1 - near)
    width = out_ref.shape[1] // members

    def far_at(step):
        return lax.rem(far + 1 + step, fars)

    def columns(block):
        return pl.ds(pl.multiple_of(block * width, width), width)

    order = [far_at(step) * 2 + (1 - near) for step in range(fars)]
    order += [far_at(step) * 2 + near for step in range(fars)]
    loads = [
        pltpu.make_async_copy(
            weight_ref.at[:, columns(block)], weight_buf.at[slot], weight_sem.at[slot]
        )
        for slot, block in enumerate(order)
    ]
    for load in loads:
        load.start()

    barrier = pltpu.get_barrier_semaphore()
    pl.semaphore_signal(barrier, inc=1, device_id={"tensor": partner}, device_id_type=MESH)
    for step in range(fars - 1):
        pl.semaphore_signal(
            barrier, inc=1, device_id={"tensor": far_at(step) * 2 + near}, device_id_type=MESH
        )
    pl.semaphore_wait(barrier, fars)

    def product(slot):
        loads[slot].wait()
        return jnp.dot(
            normalized_ref[...], weight_buf[slot], preferred_element_type=jnp.float32
        )

    def remote(source, target, sems, index, device):
        return pltpu.make_async_remote_copy(
            src_ref=source,
            dst_ref=target,
            send_sem=sems.at[0, index],
            recv_sem=sems.at[1, index],
            device_id={"tensor": device},
            device_id_type=MESH,
        )

    pair_copies = []
    for step in range(fars):
        pair_send[step] = product(step).astype(pair_send.dtype)
        copy = remote(pair_send.at[step], pair_recv.at[step], pair_sems, step, partner)
        copy.start()
        pair_copies.append(copy)
    far_copies = []
    for step in range(fars):
        summed = product(fars + step)
        pair_copies[step].wait_recv()
        summed = summed + pair_recv[step].astype(jnp.float32)
        if step < fars - 1:
            far_send[step] = summed.astype(far_send.dtype)
            copy = remote(
                far_send.at[step],
                far_recv.at[step],
                far_sems,
                step,
                far_at(step) * 2 + near,
            )
            copy.start()
            far_copies.append(copy)
        else:
            kept_acc[...] = summed
    for step in range(fars - 1):
        far_copies[step].wait_recv()
        kept_acc[...] += far_recv[step].astype(jnp.float32)
    mine = out_ref.at[:, columns(me)]
    out_ref[:, columns(me)] = kept_acc[...].astype(out_ref.dtype)
    own = remote(mine, mine, pair_out_sems, 0, partner)
    own.start()
    far_outs = []
    for step in range(fars - 1):
        copy = remote(mine, mine, far_out_sems, step, far_at(step) * 2 + near)
        copy.start()
        far_outs.append(copy)
    pair_outs = [own]
    for step in range(fars - 1):
        far_outs[step].wait_recv()
        source = lax.rem(far - 1 - step + 2 * fars, fars) * 2 + near
        there = out_ref.at[:, columns(source)]
        copy = remote(there, there, pair_out_sems, step + 1, partner)
        copy.start()
        pair_outs.append(copy)
    for copy in pair_outs:
        copy.wait_recv()
    for copy in pair_copies + far_copies + far_outs + pair_outs:
        copy.wait_send()


def project(normalized, out_weight):
    rows, inner = normalized.shape
    model_width = out_weight.shape[1]
    members = lax.axis_size("tensor")
    fars = members // 2
    width = model_width // members
    block = (rows, width)
    return pl.pallas_call(
        project_kernel,
        out_shape=jax.ShapeDtypeStruct((rows, model_width), jnp.bfloat16),
        in_specs=[
            pl.BlockSpec(memory_space=pltpu.VMEM),
            pl.BlockSpec(memory_space=pl.ANY),
        ],
        out_specs=pl.BlockSpec(memory_space=pltpu.VMEM),
        scratch_shapes=[
            pltpu.VMEM((members, inner, width), jnp.bfloat16),
            pltpu.VMEM((fars, *block), jnp.bfloat16),
            pltpu.VMEM((fars, *block), jnp.bfloat16),
            pltpu.VMEM((fars - 1, *block), jnp.bfloat16),
            pltpu.VMEM((fars - 1, *block), jnp.bfloat16),
            pltpu.VMEM(block, jnp.float32),
            pltpu.SemaphoreType.DMA((members,)),
            pltpu.SemaphoreType.DMA((2, fars)),
            pltpu.SemaphoreType.DMA((2, fars - 1)),
            pltpu.SemaphoreType.DMA((2, fars)),
            pltpu.SemaphoreType.DMA((2, fars - 1)),
        ],
        compiler_params=pltpu.CompilerParams(
            collective_id=0, has_side_effects=True, vmem_limit_bytes=40 * 1024 * 1024
        ),
    )(normalized, out_weight)


def local(
    tokens,
    norm_gain,
    in_weight,
    group_weight,
    step_weight,
    value_kernel,
    value_offset,
    group_kernel,
    group_offset,
    step_bias,
    decay_rate,
    skip_gain,
    out_gain,
    out_weight,
    scan_state,
    value_cache,
    group_cache,
    accepted,
    draft_lengths,
    live_flags,
):
    requests, positions, model_width = tokens.shape
    row_total = requests * positions
    head_count = step_bias.shape[0]
    inner_dev = value_offset.shape[0]
    head_dim = inner_dev // head_count
    tap_count = value_kernel.shape[0]
    kept_count = accepted * live_flags
    accepted_total = total_over_dp(jnp.sum(kept_count).reshape(1))
    flat_rows = tokens.reshape(row_total, model_width).astype(jnp.float32)
    normed = (
        flat_rows
        * lax.rsqrt(jnp.mean(flat_rows * flat_rows, axis=1, keepdims=True) + EPSILON)
        * norm_gain
    ).astype(jnp.bfloat16)
    parity = lax.axis_index("tensor") % 2
    in_flat = in_weight.reshape(in_weight.shape[0], 2 * inner_dev)
    inner_sum = jnp.dot(normed, in_flat, preferred_element_type=jnp.float32)
    group_sum = jnp.dot(normed, group_weight, preferred_element_type=jnp.float32)
    step_raw = jnp.dot(normed, step_weight, preferred_element_type=jnp.float32)
    inner_proj = inner_sum.astype(jnp.bfloat16).reshape(requests, positions, 2 * inner_dev)
    gate_part = inner_proj[:, :, :inner_dev]
    value_part = inner_proj[:, :, inner_dev:]
    group_proj = group_sum.astype(jnp.bfloat16).reshape(requests, positions, group_weight.shape[1])
    value_conv, value_seq = convolve(value_cache, value_part, value_kernel, value_offset)
    own_conv, group_seq = convolve(group_cache, group_proj, group_kernel, group_offset)
    other_conv = swapped(own_conv, "tensor", 0)
    input_map = jnp.where(parity == 0, own_conv, other_conv)
    output_map = jnp.where(parity == 0, other_conv, own_conv)
    values = value_conv.reshape(requests, positions, head_count, head_dim)
    step_size = jax.nn.softplus(step_raw.reshape(requests, positions, head_count) + step_bias)
    log_decay = -step_size * decay_rate
    prefix = jnp.concatenate(
        [jnp.zeros((requests, 1, head_count), jnp.float32), jnp.cumsum(log_decay, axis=1)], axis=1
    )
    after_step = prefix[:, 1:]
    alignment = jnp.einsum("rsn,rjn->rsj", narrow(output_map), narrow(input_map), preferred_element_type=jnp.float32)
    causal = (jnp.arange(positions)[:, None] >= jnp.arange(positions)[None, :])[None, :, :, None]
    spread = after_step[:, :, None, :] - after_step[:, None, :, :]
    weights_mix = (
        jnp.where(causal, jnp.exp(jnp.where(causal, spread, 0.0)), 0.0)
        * step_size[:, None, :, :]
        * alignment[:, :, :, None]
    )
    within = jnp.einsum("rsjh,rjhp->rshp", narrow(weights_mix), narrow(values), preferred_element_type=jnp.float32)
    initial = scan_state.astype(jnp.float32)
    carried = (
        jnp.einsum("rhpn,rsn->rshp", scan_state, narrow(output_map), preferred_element_type=jnp.float32)
        * jnp.exp(after_step)[:, :, :, None]
    )
    head_out = within + carried + skip_gain[:, None] * values
    one_hot = (jnp.arange(positions + 1)[None, :] == kept_count[:, None]).astype(jnp.float32)
    prefix_kept = jnp.sum(one_hot[:, :, None] * prefix, axis=1)
    before_kept = (jnp.arange(positions)[None, :] < kept_count[:, None])[:, :, None]
    keep_weight = (
        jnp.where(
            before_kept,
            jnp.exp(jnp.where(before_kept, prefix_kept[:, None, :] - after_step, 0.0)),
            0.0,
        )
        * step_size
    )
    weighted = keep_weight[:, :, :, None] * values
    kept_state = (
        jnp.exp(prefix_kept)[:, :, None, None] * initial
        + jnp.einsum("rjhp,rjn->rhpn", narrow(weighted), narrow(input_map), preferred_element_type=jnp.float32)
    ).astype(jnp.bfloat16)
    gated = head_out.reshape(row_total, inner_dev) * jax.nn.silu(
        gate_part.reshape(row_total, inner_dev).astype(jnp.float32)
    )
    own_squares = jnp.sum(gated * gated, axis=1)
    other_squares = swapped(own_squares, "tensor", 0)
    scale_rows = lax.rsqrt((own_squares + other_squares) / (2 * inner_dev) + EPSILON)
    valid_rows = (jnp.arange(positions)[None, :] < draft_lengths[:, None]) & (
        live_flags[:, None] == 1
    )
    normalized = jnp.where(
        valid_rows.reshape(row_total, 1), gated * scale_rows[:, None] * out_gain, 0.0
    ).astype(jnp.bfloat16)
    layer_rows = project(normalized, out_weight)
    value_kept = keep_window(value_seq, kept_count, tap_count - 1)
    group_kept = keep_window(group_seq, kept_count, tap_count - 1)
    return (
        layer_rows.reshape(requests, positions, model_width),
        kept_state,
        value_kept,
        group_kept,
        accepted_total,
    )


def solution(mesh):
    placed = (
        P("dp", None, None),
        P(),
        P(None, None, "tensor"),
        P(None, "tensor"),
        P(None, "tensor"),
        P(None, "tensor"),
        P("tensor"),
        P(None, "tensor"),
        P("tensor"),
        P("tensor"),
        P("tensor"),
        P("tensor"),
        P("tensor"),
        P("tensor", None),
        P("dp", "tensor", None, None),
        P("dp", None, "tensor"),
        P("dp", None, "tensor"),
        P("dp"),
        P("dp"),
        P("dp"),
    )
    return jax.shard_map(
        local,
        mesh=mesh,
        in_specs=placed,
        out_specs=(
            P("dp", None, None),
            P("dp", "tensor", None, None),
            P("dp", None, "tensor"),
            P("dp", None, "tensor"),
            P(),
        ),
        check_vma=False,
    )
```

```python
import jax
import jax.numpy as jnp
from jax import lax
from jax.experimental import pallas as pl
from jax.experimental.pallas import tpu as pltpu
from jax.sharding import PartitionSpec as P

EPSILON = 1e-05


def narrow(value):
    return value.astype(jnp.bfloat16)


def swapped(value, axis, distance):
    mask = 2**distance
    pairs = [(source, source ^ mask) for source in range(lax.axis_size(axis))]
    return lax.ppermute(value, axis, pairs)


def convolve(window, fresh_rows, kernel, offset):
    sequence = jnp.concatenate([window, fresh_rows], axis=1)
    length = fresh_rows.shape[1]
    summed = jnp.zeros(fresh_rows.shape, jnp.float32) + offset.astype(jnp.float32)
    for tap_index in range(kernel.shape[0]):
        summed = summed + kernel[tap_index].astype(jnp.float32) * sequence[
            :, tap_index : tap_index + length
        ].astype(jnp.float32)
    return (jax.nn.silu(summed), sequence)


def keep_window(sequence, kept_count, width_rows):
    kept = sequence[:, :width_rows]
    for start_row in range(1, sequence.shape[1] - width_rows + 1):
        chosen = (kept_count == start_row)[:, None, None]
        kept = jnp.where(chosen, sequence[:, start_row : start_row + width_rows], kept)
    return kept


MESH = pl.DeviceIdType.MESH


def project_kernel(
    normalized_ref,
    weight_ref,
    count_ref,
    out_ref,
    total_ref,
    weight_buf,
    pair_send,
    pair_recv,
    far_send,
    far_recv,
    kept_acc,
    count_recv,
    weight_sem,
    pair_sems,
    far_sems,
    pair_out_sems,
    far_out_sems,
    count_sems,
):
    members = lax.axis_size("tensor")
    fars = members // 2
    me = lax.axis_index("tensor")
    far, near = me // 2, me % 2
    partner = far * 2 + (1 - near)
    width = out_ref.shape[1] // members
    groups = lax.axis_size("dp")
    group = lax.axis_index("dp")
    parts, height = kept_acc.shape[:2]

    def far_at(step):
        return lax.rem(far + 1 + step, fars)

    def columns(block):
        return pl.ds(pl.multiple_of(block * width, width), width)

    order = [far_at(step) * 2 + (1 - near) for step in range(fars)]
    order += [far_at(step) * 2 + near for step in range(fars)]
    loads = [
        pltpu.make_async_copy(
            weight_ref.at[:, columns(block)], weight_buf.at[slot], weight_sem.at[slot]
        )
        for slot, block in enumerate(order)
    ]
    for load in loads:
        load.start()

    barrier = pltpu.get_barrier_semaphore()
    pl.semaphore_signal(barrier, inc=1, device_id={"tensor": partner}, device_id_type=MESH)
    for step in range(fars - 1):
        pl.semaphore_signal(
            barrier, inc=1, device_id={"tensor": far_at(step) * 2 + near}, device_id_type=MESH
        )
    for hop in range(groups - 1):
        pl.semaphore_signal(
            barrier,
            inc=1,
            device_id={"dp": lax.rem(group + 1 + hop, groups)},
            device_id_type=MESH,
        )
    pl.semaphore_wait(barrier, fars + groups - 1)

    def product(part, slot):
        if part == 0:
            loads[slot].wait()
        return jnp.dot(
            normalized_ref[part * height : (part + 1) * height],
            weight_buf[slot],
            preferred_element_type=jnp.float32,
        )

    def remote(source, target, sems, index, device):
        return pltpu.make_async_remote_copy(
            src_ref=source,
            dst_ref=target,
            send_sem=sems.at[0, index],
            recv_sem=sems.at[1, index],
            device_id={"tensor": device},
            device_id_type=MESH,
        )

    count_copies = []
    for hop in range(groups - 1):
        copy = pltpu.make_async_remote_copy(
            src_ref=count_ref,
            dst_ref=count_recv.at[hop],
            send_sem=count_sems.at[0, hop],
            recv_sem=count_sems.at[1, hop],
            device_id={"dp": lax.rem(group + 1 + hop, groups)},
            device_id_type=MESH,
        )
        copy.start()
        count_copies.append(copy)

    pair_copies, far_copies, pair_outs, far_outs = [], [], [], []
    for part in range(parts):
        for step in range(fars):
            slot = part * fars + step
            pair_send[slot] = product(part, step).astype(pair_send.dtype)
            copy = remote(pair_send.at[slot], pair_recv.at[slot], pair_sems, slot, partner)
            copy.start()
            pair_copies.append(copy)
    for part in range(parts):
        for step in range(fars):
            summed = product(part, fars + step)
            pair_copies[part * fars + step].wait_recv()
            summed = summed + pair_recv[part * fars + step].astype(jnp.float32)
            if step < fars - 1:
                slot = part * (fars - 1) + step
                far_send[slot] = summed.astype(far_send.dtype)
                copy = remote(
                    far_send.at[slot],
                    far_recv.at[slot],
                    far_sems,
                    slot,
                    far_at(step) * 2 + near,
                )
                copy.start()
                far_copies.append(copy)
            else:
                kept_acc[part] = summed
    for part in range(parts):
        rows = pl.ds(part * height, height)
        total = kept_acc[part]
        for step in range(fars - 1):
            slot = part * (fars - 1) + step
            far_copies[slot].wait_recv()
            total = total + far_recv[slot].astype(jnp.float32)
        mine = out_ref.at[rows, columns(me)]
        out_ref[rows, columns(me)] = total.astype(out_ref.dtype)
        copy = remote(mine, mine, pair_out_sems, part * fars, partner)
        copy.start()
        pair_outs.append(copy)
        for step in range(fars - 1):
            slot = part * (fars - 1) + step
            copy = remote(mine, mine, far_out_sems, slot, far_at(step) * 2 + near)
            copy.start()
            far_outs.append(copy)
    for part in range(parts):
        rows = pl.ds(part * height, height)
        for step in range(fars - 1):
            far_outs[part * (fars - 1) + step].wait_recv()
            source = lax.rem(far - 1 - step + 2 * fars, fars) * 2 + near
            there = out_ref.at[rows, columns(source)]
            copy = remote(there, there, pair_out_sems, part * fars + step + 1, partner)
            copy.start()
            pair_outs.append(copy)
    count = count_ref[...]
    for hop in range(groups - 1):
        count_copies[hop].wait_recv()
        count = count + count_recv[hop]
    total_ref[...] = count
    for copy in pair_outs:
        copy.wait_recv()
    for copy in pair_copies + far_copies + far_outs + pair_outs + count_copies:
        copy.wait_send()


def project(normalized, out_weight, own_total):
    rows, inner = normalized.shape
    model_width = out_weight.shape[1]
    members = lax.axis_size("tensor")
    groups = lax.axis_size("dp")
    fars = members // 2
    parts = 2 if rows % 32 == 0 else 1
    width = model_width // members
    block = (rows // parts, width)
    return pl.pallas_call(
        project_kernel,
        out_shape=[
            jax.ShapeDtypeStruct((rows, model_width), jnp.bfloat16),
            jax.ShapeDtypeStruct(own_total.shape, jnp.int32),
        ],
        in_specs=[
            pl.BlockSpec(memory_space=pltpu.VMEM),
            pl.BlockSpec(memory_space=pl.ANY),
            pl.BlockSpec(memory_space=pltpu.VMEM),
        ],
        out_specs=[pl.BlockSpec(memory_space=pltpu.VMEM)] * 2,
        scratch_shapes=[
            pltpu.VMEM((members, inner, width), jnp.bfloat16),
            pltpu.VMEM((parts * fars, *block), jnp.bfloat16),
            pltpu.VMEM((parts * fars, *block), jnp.bfloat16),
            pltpu.VMEM((parts * (fars - 1), *block), jnp.bfloat16),
            pltpu.VMEM((parts * (fars - 1), *block), jnp.bfloat16),
            pltpu.VMEM((parts, *block), jnp.float32),
            pltpu.VMEM((groups - 1, *own_total.shape), jnp.int32),
            pltpu.SemaphoreType.DMA((members,)),
            pltpu.SemaphoreType.DMA((2, parts * fars)),
            pltpu.SemaphoreType.DMA((2, parts * (fars - 1))),
            pltpu.SemaphoreType.DMA((2, parts * fars)),
            pltpu.SemaphoreType.DMA((2, parts * (fars - 1))),
            pltpu.SemaphoreType.DMA((2, groups - 1)),
        ],
        compiler_params=pltpu.CompilerParams(
            collective_id=0, has_side_effects=True, vmem_limit_bytes=40 * 1024 * 1024
        ),
    )(normalized, out_weight, own_total)


def local(
    tokens,
    norm_gain,
    in_weight,
    group_weight,
    step_weight,
    value_kernel,
    value_offset,
    group_kernel,
    group_offset,
    step_bias,
    decay_rate,
    skip_gain,
    out_gain,
    out_weight,
    scan_state,
    value_cache,
    group_cache,
    accepted,
    draft_lengths,
    live_flags,
):
    requests, positions, model_width = tokens.shape
    row_total = requests * positions
    head_count = step_bias.shape[0]
    inner_dev = value_offset.shape[0]
    head_dim = inner_dev // head_count
    tap_count = value_kernel.shape[0]
    kept_count = accepted * live_flags
    wide = tokens.astype(jnp.float32)
    normed = (
        (wide * lax.rsqrt(jnp.mean(wide * wide, axis=2, keepdims=True) + EPSILON) * norm_gain)
        .astype(jnp.bfloat16)
        .reshape(row_total, model_width)
    )
    parity = lax.axis_index("tensor") % 2
    inner_sum = jnp.einsum("rd,dgi->rgi", normed, in_weight, preferred_element_type=jnp.float32)
    group_sum = jnp.dot(normed, group_weight, preferred_element_type=jnp.float32)
    step_raw = jnp.dot(normed, step_weight, preferred_element_type=jnp.float32)
    inner_proj = inner_sum.astype(jnp.bfloat16).reshape(requests, positions, 2 * inner_dev)
    gate_part = inner_proj[:, :, :inner_dev]
    value_part = inner_proj[:, :, inner_dev:]
    group_proj = group_sum.astype(jnp.bfloat16).reshape(requests, positions, group_weight.shape[1])
    value_conv, value_seq = convolve(value_cache, value_part, value_kernel, value_offset)
    own_conv, group_seq = convolve(group_cache, group_proj, group_kernel, group_offset)
    other_conv = swapped(own_conv, "tensor", 0)
    input_map = jnp.where(parity == 0, own_conv, other_conv)
    output_map = jnp.where(parity == 0, other_conv, own_conv)
    values = value_conv.reshape(requests, positions, head_count, head_dim)
    step_size = jax.nn.softplus(step_raw.reshape(requests, positions, head_count) + step_bias)
    log_decay = -step_size * decay_rate
    prefix = jnp.concatenate(
        [jnp.zeros((requests, 1, head_count), jnp.float32), jnp.cumsum(log_decay, axis=1)], axis=1
    )
    after_step = prefix[:, 1:]
    alignment = jnp.einsum("rsn,rjn->rsj", narrow(output_map), narrow(input_map), preferred_element_type=jnp.float32)
    causal = (jnp.arange(positions)[:, None] >= jnp.arange(positions)[None, :])[None, :, :, None]
    spread = after_step[:, :, None, :] - after_step[:, None, :, :]
    weights_mix = (
        jnp.where(causal, jnp.exp(jnp.where(causal, spread, 0.0)), 0.0)
        * step_size[:, None, :, :]
        * alignment[:, :, :, None]
    )
    within = jnp.einsum("rsjh,rjhp->rshp", narrow(weights_mix), narrow(values), preferred_element_type=jnp.float32)
    initial = scan_state.astype(jnp.float32)
    carried = (
        jnp.einsum("rhpn,rsn->rshp", scan_state, narrow(output_map), preferred_element_type=jnp.float32)
        * jnp.exp(after_step)[:, :, :, None]
    )
    head_out = within + carried + skip_gain[:, None] * values
    one_hot = (jnp.arange(positions + 1)[None, :] == kept_count[:, None]).astype(jnp.float32)
    prefix_kept = jnp.sum(one_hot[:, :, None] * prefix, axis=1)
    before_kept = (jnp.arange(positions)[None, :] < kept_count[:, None])[:, :, None]
    keep_weight = (
        jnp.where(
            before_kept,
            jnp.exp(jnp.where(before_kept, prefix_kept[:, None, :] - after_step, 0.0)),
            0.0,
        )
        * step_size
    )
    weighted = keep_weight[:, :, :, None] * values
    kept_state = (
        jnp.exp(prefix_kept)[:, :, None, None] * initial
        + jnp.einsum("rjhp,rjn->rhpn", narrow(weighted), narrow(input_map), preferred_element_type=jnp.float32)
    ).astype(jnp.bfloat16)
    gated = head_out.reshape(requests, positions, inner_dev) * jax.nn.silu(
        gate_part.astype(jnp.float32)
    )
    own_squares = jnp.sum(gated * gated, axis=2)
    other_squares = swapped(own_squares, "tensor", 0)
    scale_rows = lax.rsqrt((own_squares + other_squares) / (2 * inner_dev) + EPSILON)
    valid_rows = (jnp.arange(positions)[None, :] < draft_lengths[:, None]) & (
        live_flags[:, None] == 1
    )
    normalized = (
        jnp.where(valid_rows[:, :, None], gated * scale_rows[:, :, None] * out_gain, 0.0)
        .astype(jnp.bfloat16)
        .reshape(row_total, inner_dev)
    )
    own_total = jnp.broadcast_to(jnp.sum(kept_count), (8, 128))
    layer_rows, totals = project(normalized, out_weight, own_total)
    accepted_total = totals[0, :1]
    value_kept = keep_window(value_seq, kept_count, tap_count - 1)
    group_kept = keep_window(group_seq, kept_count, tap_count - 1)
    return (
        layer_rows.reshape(requests, positions, model_width),
        kept_state,
        value_kept,
        group_kept,
        accepted_total,
    )


def solution(mesh):
    placed = (
        P("dp", None, None),
        P(),
        P(None, None, "tensor"),
        P(None, "tensor"),
        P(None, "tensor"),
        P(None, "tensor"),
        P("tensor"),
        P(None, "tensor"),
        P("tensor"),
        P("tensor"),
        P("tensor"),
        P("tensor"),
        P("tensor"),
        P("tensor", None),
        P("dp", "tensor", None, None),
        P("dp", None, "tensor"),
        P("dp", None, "tensor"),
        P("dp"),
        P("dp"),
        P("dp"),
    )
    return jax.shard_map(
        local,
        mesh=mesh,
        in_specs=placed,
        out_specs=(
            P("dp", None, None),
            P("dp", "tensor", None, None),
            P("dp", None, "tensor"),
            P("dp", None, "tensor"),
            P(),
        ),
        check_vma=False,
    )
```
